512 devices in a mesh: groups: 2 (over y), row: 16 (over z), col: 16 (over x, core).
Axes of the slice: x: 8, y: 2, z: 16, core: 2. Of those that a mesh axis runs over, the one named last changes fastest.
The devices are a block of a 8x8x16 slice.
Arguments:
- activations: bfloat16 [3072, 4096], P(('groups', 'row'), 'col'), parts along dimension 0, may hold values from -52 to 52
- damping: float32 [8192], P(('groups', 'row')), parts along dimension 0, may hold values from 0.1 to 1
Outputs:
- factor: float32 [8192, 4096], P(('groups', 'row'), 'col'), parts along dimension 0
The draws below stay inside these ranges and needn't reach their ends.
There are 2 independent parts, one for each index of `groups`. The reference program is written for one: setup_inputs(seed, part) draws one part's arguments, and reference() takes and returns one part's arrays. A program takes and returns all parts, laid end to end along the dimension named above; each array names one. Nothing has to cross between parts.
All inputs are finite; a program needn't handle non-finite values.
Results may differ from the reference program's by a relative error of at most 0.0003.
Values may be sent and summed in bfloat16 or wider, within the bound.
No kernel may reach another device: no remote copies, remote signals or barrier semaphores. Data moves between devices by JAX's collectives and lax.ppermute only.
A program may use at most 64 MiB of HBM per device.

```python
import math
import jax
import jax.numpy as jnp
from jax import lax

D = 4096
NB = 256
PANELS = 2
TOKENS = 1536


def draw_activations(key, part):
    draw_keys = jax.random.split(key, 5)
    row_scale = jnp.exp(jax.random.uniform(draw_keys[0], (TOKENS, 1), jnp.float32, math.log(0.3), math.log(3.0)))
    col_scale = jnp.exp(jax.random.uniform(draw_keys[1], (1, D), jnp.float32, math.log(0.3), math.log(3.0)))
    first_perm = jax.random.permutation(draw_keys[2], D)
    second_perm = jax.random.permutation(draw_keys[3], D)
    base_draw = jnp.clip(jax.random.normal(draw_keys[4], (TOKENS, D), jnp.float32), -4.0, 4.0)
    mixed = base_draw + 0.6 * base_draw[:, first_perm] + 0.4 * base_draw[:, second_perm]
    return (mixed * row_scale * col_scale / 1.4).astype(jnp.bfloat16)


def steps_of(stream_key, shape, cuts, smallest, top_value):
    def one(position, blocks):
        draws = jax.random.uniform(jax.random.fold_in(jax.random.fold_in(stream_key, 6), position), (blocks,), jnp.float32, smallest / len(cuts), top_value / len(cuts))
        return jnp.repeat(jnp.exp(draws), shape[position] // blocks).reshape((-1,) + (1,) * (len(shape) - position - 1))

    level = one(*cuts[0])
    for cut in cuts[1:]:
        level = level * one(*cut)
    return level


def setup_inputs(seed: int = 0, part: int = 0) -> dict:
    key_of = jax.random.split(jax.random.key(seed), 3)
    own_keys = jax.random.split(jax.random.fold_in(key_of[2], part), 3)
    activations = draw_activations(jax.random.fold_in(jax.random.fold_in(key_of[2], part), 71), part)
    damping = jnp.clip(jnp.exp(math.log(1.0) - 2.3025851 * jax.random.uniform(own_keys[1], (D,), jnp.float32) ** steps_of(own_keys[1], (D,), ((0, 16),), -0.2, 0.2)), 0.1, 1.0)
    return {"activations": activations, "damping": damping}


def reference(activations, damping):
    gram = lax.dot_general(activations.astype(jnp.float32), activations.astype(jnp.float32), (((0,), (0,)), ((), ())), preferred_element_type=jnp.float32)
    matrix = gram / TOKENS + jnp.diag(damping)
    for panel_index in range(PANELS):
        begin_at = panel_index * NB
        end_at = begin_at + NB
        pivot_block = jnp.linalg.cholesky(matrix[begin_at:end_at, begin_at:end_at])
        panel_rows = jax.scipy.linalg.solve_triangular(pivot_block, matrix[end_at:, begin_at:end_at].T, lower=True).T
        update = jnp.dot(panel_rows.astype(jnp.float32), panel_rows.T.astype(jnp.float32), precision=lax.Precision.HIGHEST, preferred_element_type=jnp.float32)
        matrix = matrix.at[end_at:, end_at:].add(-update)
        matrix = matrix.at[begin_at:end_at, begin_at:end_at].set(pivot_block)
        matrix = matrix.at[end_at:, begin_at:end_at].set(panel_rows)
        matrix = matrix.at[begin_at:end_at, end_at:].set(0.0)
    return matrix
```

```python
import jax
import jax.numpy as jnp
from jax import lax
from jax.experimental import pallas as pl
from jax.experimental.pallas import tpu as pltpu
from jax.sharding import PartitionSpec as P

NB = 256
PANELS = 2
LEAD = NB * PANELS
BS = 128
SUB = 8

HIGHEST = lax.Precision.HIGHEST


def tdot(a, b, precision=None):
    return lax.dot_general(
        a, b, (((0,), (0,)), ((), ())), precision=precision, preferred_element_type=jnp.float32
    )


def factor_block(g_ref):
    sub = lax.broadcasted_iota(jnp.int32, (SUB, 2 * BS), 0)
    strips = BS // SUB
    for k in range(strips):
        rows = [g_ref[i * SUB : (i + 1) * SUB, :] for i in range(k, strips)]
        cols = [
            [jnp.broadcast_to(g[:, SUB * k + j : SUB * k + j + 1], (SUB, BS)) for j in range(SUB)]
            for g in rows
        ]
        done = []
        for j in range(SUB):
            d = jnp.broadcast_to(cols[0][j][j : j + 1, :], (SUB, BS))
            rs = lax.rsqrt(d)
            rs = rs * (1.5 - 0.5 * d * rs * rs)
            low = [c[j] * rs for c in cols]
            u = jnp.broadcast_to(rows[0][j : j + 1, :], (SUB, 2 * BS)) * jnp.concatenate([rs, rs], 1)
            done.append(u)
            for m in range(j + 1, SUB):
                c = jnp.broadcast_to(low[0][m : m + 1, :], (SUB, BS))
                for i in range(len(rows)):
                    cols[i][m] = cols[i][m] - low[i] * c
            for i in range(len(rows)):
                rows[i] = rows[i] - jnp.concatenate([low[i], low[i]], 1) * u
        out = done[SUB - 1]
        for j in range(SUB - 1):
            out = jnp.where(sub == j, done[j], out)
        g_ref[SUB * k : SUB * (k + 1), :] = out
        for i in range(1, len(rows)):
            g_ref[(k + i) * SUB : (k + i + 1) * SUB, :] = rows[i]


def local_kernel(at_ref, lead_ref, ar_ref, ac_ref, dlead_ref, down_ref, o_ref, w_ref, u_ref, g_ref, *, scale):
    r = at_ref[0]
    c = at_ref[1]
    width = LEAD + 2 * NB

    def eye(n):
        i = lax.broadcasted_iota(jnp.int32, (n, n), 0)
        j = lax.broadcasted_iota(jnp.int32, (n, n), 1)
        return i == j

    lead = lead_ref[...]
    w_ref[:, :LEAD] = tdot(lead, lead) * scale + jnp.where(eye(LEAD), dlead_ref[...], 0.0)
    w_ref[:, LEAD : LEAD + NB] = tdot(lead, ar_ref[...]) * scale
    w_ref[:, LEAD + NB :] = tdot(lead, ac_ref[...]) * scale

    steps = LEAD // BS

    def step(b, carry):
        at = pl.multiple_of(b * BS, BS)
        for k in range(steps):
            @pl.when(b == k)
            def _():
                g_ref[:, :BS] = w_ref[k * BS : (k + 1) * BS, k * BS : (k + 1) * BS]
        g_ref[:, BS:] = jnp.where(eye(BS), 1.0, 0.0).astype(jnp.float32)
        factor_block(g_ref)
        u = jnp.dot(
            g_ref[:, BS:], w_ref[pl.ds(at, BS), :], precision=HIGHEST, preferred_element_type=jnp.float32
        )
        u_ref[pl.ds(at, BS), :] = u
        for k in range(steps):
            @pl.when(b == k)
            def _():
                u_ref[k * BS : (k + 1) * BS, k * BS : (k + 1) * BS] = g_ref[:, :BS]
                for m in range(k + 1, steps):
                    w_ref[m * BS : (m + 1) * BS, :] -= tdot(u[:, m * BS : (m + 1) * BS], u, HIGHEST)
        return carry

    lax.fori_loop(0, steps, step, 0)

    i = lax.broadcasted_iota(jnp.int32, (NB, NB), 0)
    j = lax.broadcasted_iota(jnp.int32, (NB, NB), 1)

    @pl.when((c >= PANELS) & (r >= PANELS))
    def _():
        own = tdot(ar_ref[...], ac_ref[...]) * scale
        own = own + jnp.where((i == j) & (r == c), down_ref[...], 0.0)
        o_ref[...] = own - tdot(u_ref[:, LEAD : LEAD + NB], u_ref[:, LEAD + NB :], HIGHEST)

    @pl.when((r < PANELS) & (c > r))
    def _():
        o_ref[...] = jnp.zeros((NB, NB), jnp.float32)

    for p in range(PANELS):
        @pl.when((c == p) & (r == p))
        def _():
            o_ref[...] = jnp.where(i >= j, u_ref[p * NB : (p + 1) * NB, p * NB : (p + 1) * NB].T, 0.0)

        @pl.when((c == p) & (r > p))
        def _():
            o_ref[...] = u_ref[p * NB : (p + 1) * NB, LEAD : LEAD + NB].T


def local_part(at, lead, rows, cols, dlead, down, scale):
    import functools

    vmem = pl.BlockSpec(memory_space=pltpu.VMEM)
    return pl.pallas_call(
        functools.partial(local_kernel, scale=scale),
        out_shape=jax.ShapeDtypeStruct((NB, NB), jnp.float32),
        in_specs=[pl.BlockSpec(memory_space=pltpu.SMEM)] + [vmem] * 5,
        out_specs=vmem,
        scratch_shapes=[
            pltpu.VMEM((LEAD, LEAD + 2 * NB), jnp.float32),
            pltpu.VMEM((LEAD, LEAD + 2 * NB), jnp.float32),
            pltpu.VMEM((BS, 2 * BS), jnp.float32),
        ],
    )(at, lead, rows, cols, dlead, down)


def to_all(shard, axis, copies, groups=None):
    shards = jnp.broadcast_to(shard, (copies, *shard.shape))
    return lax.all_to_all(shards, axis, 0, 0, axis_index_groups=groups, tiled=True)


def on_device(activations, damping):
    tokens, width = activations.shape
    grid = lax.axis_size("row")
    cores = 2
    chips = lax.axis_size("col") // cores
    piece = tokens // chips
    row_dev = lax.axis_index("row")
    col_dev = lax.axis_index("col")
    core = col_dev % cores
    same_core = [[x * cores + k for x in range(chips)] for k in range(cores)]
    transpose = [(r * grid + c, c * grid + r) for r in range(grid) for c in range(grid)]

    turned = lax.ppermute(activations, ("row", "col"), transpose)
    lead_piece = lax.all_to_all(
        activations.reshape(chips, piece, width), "col", 0, 0, axis_index_groups=same_core, tiled=True
    )[0]

    d0 = lax.reduce_precision(damping, 8, 7)
    d1 = lax.reduce_precision(damping - d0, 8, 7)
    d2 = damping - d0 - d1
    damp_rows = jnp.stack([d0, d1, d2, jnp.zeros_like(d2)]).astype(jnp.bfloat16)
    sent = jnp.concatenate([activations, lead_piece, damp_rows])
    got = lax.all_gather(sent, "row")
    cols = got[:, :tokens]
    lead_pieces = got[:, tokens : tokens + piece].reshape(grid * piece, width)
    damp = got[:PANELS, tokens + piece :].astype(jnp.float32)
    damp = ((damp[:, 2] + damp[:, 1]) + damp[:, 0]).reshape(1, PANELS * width)

    sent = jnp.concatenate([lead_pieces, turned])
    mine = to_all(sent, "col", chips, same_core)
    other = lax.ppermute(mine, "col", [(c, c ^ 1) for c in range(chips * cores)])
    first = jnp.where(core == 0, mine, other)
    second = jnp.where(core == 0, other, mine)
    n = grid * piece
    lead = jnp.concatenate([first[:, :n].reshape(chips * n, width), second[:, :n].reshape(chips * n, width)], 1)
    rows = jnp.stack([first[:, n:], second[:, n:]], 1)

    def in_lead_order(x):
        return x.reshape(grid, chips, piece, width).transpose(1, 0, 2, 3).reshape(grid * tokens, width)

    at = jnp.stack([row_dev, col_dev]).astype(jnp.int32)
    return local_part(
        at, lead, in_lead_order(rows), in_lead_order(cols), damp, damping.reshape(1, width), 1.0 / (tokens * grid)
    )


def solution(mesh):
    in_specs = (P(("groups", "row"), "col"), P(("groups", "row")))
    out_specs = P(("groups", "row"), "col")
    return jax.shard_map(
        on_device, mesh=mesh, in_specs=in_specs, out_specs=out_specs, check_vma=False
    )
```

```python
import functools

import jax
import jax.numpy as jnp
from jax import lax
from jax.experimental import pallas as pl
from jax.experimental.pallas import tpu as pltpu
from jax.sharding import PartitionSpec as P


NB = 256
PANELS = 2
LEAD = NB * PANELS
BS = 128
SUB = 8

HIGHEST = lax.Precision.HIGHEST


def tdot(a, b, precision=None):
    return lax.dot_general(
        a, b, (((0,), (0,)), ((), ())), precision=precision, preferred_element_type=jnp.float32
    )


def both(x):
    return jnp.concatenate([x, x], 1)


def factor_block(g_ref):
    sub = lax.broadcasted_iota(jnp.int32, (SUB, BS), 0)
    sub2 = lax.broadcasted_iota(jnp.int32, (SUB, 2 * BS), 0)
    strips = BS // SUB
    for k in range(strips):
        at = SUB * k
        rows = g_ref[at : at + SUB, :]
        cols = [jnp.broadcast_to(rows[:, at + j : at + j + 1], (SUB, BS)) for j in range(SUB)]
        piv = [[jnp.broadcast_to(cols[j][m : m + 1, :], (SUB, BS)) for j in range(m + 1)] for m in range(SUB)]
        out = rows
        for j in range(SUB):
            rc = 1.0 / piv[j][j]
            rs = lax.rsqrt(piv[j][j])
            t = {m: piv[m][j] * rc for m in range(j + 1, SUB)}
            for m in range(j + 1, SUB):
                for n in range(m, SUB):
                    piv[n][m] = piv[n][m] - piv[n][j] * t[m]
                cols[m] = jnp.where(sub == j, t[m], cols[m] - cols[j] * t[m])
            row = jnp.broadcast_to(rows[j : j + 1, :], (SUB, 2 * BS))
            out = jnp.where(sub2 == j, row * both(rs), out)
            w = row * both(rc)
            rows = jnp.where(sub2 == j, w, rows - both(cols[j]) * w)
        g_ref[at : at + SUB, :] = out
        if k + 1 < strips:
            solved = [jnp.broadcast_to(rows[j : j + 1, :], (SUB, 2 * BS)) for j in range(SUB)]
            for i in range(k + 1, strips):
                g = g_ref[i * SUB : (i + 1) * SUB, :]
                acc = g
                for j in range(SUB):
                    acc = acc - both(jnp.broadcast_to(g[:, at + j : at + j + 1], (SUB, BS))) * solved[j]
                g_ref[i * SUB : (i + 1) * SUB, :] = acc


def local_kernel(
    at_ref, mine_ref, other_ref, cols_ref, dlead_ref, down_ref, o_ref,
    lead_ref, ar_ref, ac_ref, w_ref, u_ref, g_ref, *, scale, quarters,
):
    r = at_ref[0]
    c = at_ref[1]
    even = at_ref[2] == 0
    grid, tokens, _ = cols_ref.shape
    part = tokens // quarters
    block = grid * part

    def eye(n):
        i = lax.broadcasted_iota(jnp.int32, (n, n), 0)
        j = lax.broadcasted_iota(jnp.int32, (n, n), 1)
        return i == j

    for q in range(quarters):
        for h in range(2):
            x = h * quarters + q
            mine = mine_ref[x, :block, :]
            other = other_ref[x, :block, :]
            lead_ref[q * block : (q + 1) * block, h * BS : (h + 1) * BS] = jnp.where(even, mine, other)
            lead_ref[q * block : (q + 1) * block, NB + h * BS : NB + (h + 1) * BS] = jnp.where(even, other, mine)
    for t in range(grid):
        for q in range(quarters):
            to = slice(q * block + t * part, q * block + (t + 1) * part)
            ac_ref[to, :] = cols_ref[t, q * part : (q + 1) * part, :]
            for h in range(2):
                at = block + h * tokens + q * part
                mine = mine_ref[t // 2, at : at + part, :]
                other = other_ref[t // 2, at : at + part, :]
                same = even if t % 2 == 0 else jnp.logical_not(even)
                ar_ref[to, h * BS : (h + 1) * BS] = jnp.where(same, mine, other)

    lead = lead_ref[...]
    w_ref[:, :LEAD] = tdot(lead, lead) * scale + jnp.where(eye(LEAD), dlead_ref[...], 0.0)
    w_ref[:, LEAD : LEAD + NB] = tdot(lead, ar_ref[...]) * scale
    w_ref[:, LEAD + NB :] = tdot(lead, ac_ref[...]) * scale

    steps = LEAD // BS

    def step(b, carry):
        for k in range(steps):
            @pl.when(b == k)
            def _():
                g_ref[:, :BS] = w_ref[k * BS : (k + 1) * BS, k * BS : (k + 1) * BS]
        g_ref[:, BS:] = jnp.where(eye(BS), 1.0, 0.0).astype(jnp.float32)
        factor_block(g_ref)
        for k in range(steps):
            @pl.when(b == k)
            def _():
                here = slice(k * BS, (k + 1) * BS)
                after = (k + 1) * BS
                u = jnp.dot(
                    g_ref[:, BS:], w_ref[here, after:], precision=HIGHEST, preferred_element_type=jnp.float32
                )
                u_ref[here, here] = g_ref[:, :BS]
                u_ref[here, after:] = u
                if after < LEAD:
                    w_ref[after:LEAD, after:] -= tdot(u[:, : LEAD - after], u, HIGHEST)
        return carry

    lax.fori_loop(0, steps, step, 0)

    i = lax.broadcasted_iota(jnp.int32, (NB, NB), 0)
    j = lax.broadcasted_iota(jnp.int32, (NB, NB), 1)

    @pl.when((c >= PANELS) & (r >= PANELS))
    def _():
        own = tdot(ar_ref[...], ac_ref[...]) * scale
        own = own + jnp.where((i == j) & (r == c), down_ref[...], 0.0)
        o_ref[...] = own - tdot(u_ref[:, LEAD : LEAD + NB], u_ref[:, LEAD + NB :], HIGHEST)

    @pl.when((r < PANELS) & (c > r))
    def _():
        o_ref[...] = jnp.zeros((NB, NB), jnp.float32)

    for p in range(PANELS):
        here = slice(p * NB, (p + 1) * NB)

        @pl.when((c == p) & (r == p))
        def _():
            o_ref[:BS, :BS] = u_ref[p * NB : p * NB + BS, p * NB : p * NB + BS].T
            o_ref[:BS, BS:] = jnp.zeros((BS, BS), jnp.float32)
            o_ref[BS:, :BS] = u_ref[p * NB : p * NB + BS, p * NB + BS : (p + 1) * NB].T
            o_ref[BS:, BS:] = u_ref[p * NB + BS : (p + 1) * NB, p * NB + BS : (p + 1) * NB].T
            o_ref[...] = jnp.where(i >= j, o_ref[...], 0.0)

        @pl.when((c == p) & (r > p))
        def _():
            o_ref[...] = u_ref[here, LEAD : LEAD + NB].T


def local_part(at, mine, other, cols, dlead, down, scale, quarters):
    vmem = pl.BlockSpec(memory_space=pltpu.VMEM)
    total = cols.shape[0] * cols.shape[1]
    return pl.pallas_call(
        functools.partial(local_kernel, scale=scale, quarters=quarters),
        out_shape=jax.ShapeDtypeStruct((NB, NB), jnp.float32),
        in_specs=[pl.BlockSpec(memory_space=pltpu.SMEM)] + [vmem] * 5,
        out_specs=vmem,
        scratch_shapes=[
            pltpu.VMEM((total, LEAD), jnp.bfloat16),
            pltpu.VMEM((total, NB), jnp.bfloat16),
            pltpu.VMEM((total, NB), jnp.bfloat16),
            pltpu.VMEM((LEAD, LEAD + 2 * NB), jnp.float32),
            pltpu.VMEM((LEAD, LEAD + 2 * NB), jnp.float32),
            pltpu.VMEM((BS, 2 * BS), jnp.float32),
        ],
    )(at, mine, other, cols, dlead, down)


def to_all(shard, axis, copies, groups=None):
    shards = jnp.broadcast_to(shard, (copies, *shard.shape))
    return lax.all_to_all(shards, axis, 0, 0, axis_index_groups=groups, tiled=True)


def on_device(activations, damping):
    tokens, width = activations.shape
    grid = lax.axis_size("row")
    cores = 2
    chips = lax.axis_size("col") // cores
    halves = width // BS
    quarters = chips // halves
    part = tokens // quarters
    row_dev = lax.axis_index("row")
    col_dev = lax.axis_index("col")
    core = col_dev % cores
    same_core = [[x * cores + k for x in range(chips)] for k in range(cores)]
    transpose = [(r * grid + c, c * grid + r) for r in range(grid) for c in range(grid)]

    def by_half(x):
        return x.reshape(tokens, halves, BS).transpose(1, 0, 2)

    turned = lax.ppermute(activations, ("row", "col"), transpose)
    lead_piece = lax.all_to_all(
        by_half(activations).reshape(chips, part, BS), "col", 0, 0, axis_index_groups=same_core, tiled=True
    )[0]

    d0 = lax.reduce_precision(damping, 8, 7)
    d1 = lax.reduce_precision(damping - d0, 8, 7)
    d2 = damping - d0 - d1
    damp_rows = jnp.stack([d0, d1, d2, jnp.zeros_like(d2)]).astype(jnp.bfloat16).reshape(4 * halves, BS)
    pieces = to_all(jnp.concatenate([lead_piece, damp_rows]), "row", grid)
    damp = pieces[:PANELS, part:].reshape(PANELS, 4, width).astype(jnp.float32)
    damp = ((damp[:, 2] + damp[:, 1]) + damp[:, 0]).reshape(1, PANELS * width)

    own, pieces = lax.optimization_barrier((activations, pieces))
    sent = jnp.concatenate([pieces[:, :part].reshape(grid * part, BS), by_half(turned).reshape(halves * tokens, BS)])
    mine = to_all(sent, "col", chips, same_core)
    cols = lax.all_gather(own, "row")
    other = lax.ppermute(mine, "col", [(c, c ^ 1) for c in range(chips * cores)])
    at = jnp.stack([row_dev, col_dev, core]).astype(jnp.int32)
    return local_part(
        at, mine, other, cols, damp, damping.reshape(1, width), 1.0 / (tokens * grid), quarters
    )


def solution(mesh):
    in_specs = (P(("groups", "row"), "col"), P(("groups", "row")))
    out_specs = P(("groups", "row"), "col")
    return jax.shard_map(
        on_device, mesh=mesh, in_specs=in_specs, out_specs=out_specs, check_vma=False
    )
```

```python
import functools

import jax
import jax.numpy as jnp
from jax import lax
from jax.experimental import pallas as pl
from jax.experimental.pallas import tpu as pltpu
from jax.sharding import PartitionSpec as P


NB = 256
PANELS = 2
LEAD = NB * PANELS
BS = 128
SUB = 8

HIGHEST = lax.Precision.HIGHEST


def tdot(a, b, precision=None):
    return lax.dot_general(
        a, b, (((0,), (0,)), ((), ())), precision=precision, preferred_element_type=jnp.float32
    )


def both(x):
    return jnp.concatenate([x, x], 1)


def lanes(g, at):
    return [jnp.broadcast_to(g[:, at + j : at + j + 1], (SUB, BS)) for j in range(SUB)]


def sublane(x, m):
    return jnp.broadcast_to(x[m : m + 1, :], (SUB, x.shape[1]))


def factor_block(g_ref):
    sub = lax.broadcasted_iota(jnp.int32, (SUB, BS), 0)
    sub2 = lax.broadcasted_iota(jnp.int32, (SUB, 2 * BS), 0)
    strips = BS // SUB
    half = strips // 2
    for k in range(strips):
        at = SUB * k
        end = (k // half + 1) * half
        if k % half == 0:
            if k > 0:
                g_ref[at:, :] -= tdot(g_ref[:at, at:BS], g_ref[:at, :], HIGHEST)
            rows = g_ref[at : at + SUB, :]
            cols = lanes(rows, at)
        ahead = k + 1 < end
        if ahead:
            next_rows = g_ref[at + SUB : at + 2 * SUB, :]
            low = lanes(next_rows, at)
            next_cols = lanes(next_rows, at + SUB)
        out = rows
        for j in range(SUB):
            d = sublane(cols[j], j)
            rc = 1.0 / d
            rs = lax.rsqrt(d)
            t = {m: sublane(cols[j], m) * rc for m in range(j + 1, SUB)}
            if ahead:
                for n in range(SUB):
                    next_cols[n] = next_cols[n] - low[j] * (sublane(low[j], n) * rc)
                for m in range(j + 1, SUB):
                    low[m] = low[m] - low[j] * t[m]
            for m in range(j + 1, SUB):
                cols[m] = jnp.where(sub == j, t[m], cols[m] - cols[j] * t[m])
            row = sublane(rows, j)
            out = jnp.where(sub2 == j, row * both(rs), out)
            w = row * both(rc)
            rows = jnp.where(sub2 == j, w, rows - both(cols[j]) * w)
            if ahead:
                next_rows = next_rows - both(low[j]) * w
        g_ref[at : at + SUB, :] = out
        if k + 2 < end:
            solved = [sublane(rows, j) for j in range(SUB)]
            for i in range(k + 2, end):
                acc = g_ref[i * SUB : (i + 1) * SUB, :]
                for a, y in zip(lanes(acc, at), solved, strict=True):
                    acc = acc - both(a) * y
                g_ref[i * SUB : (i + 1) * SUB, :] = acc
        if ahead:
            rows, cols = next_rows, next_cols


def local_kernel(
    at_ref, mine_ref, other_ref, cols_ref, dlead_ref, down_ref, o_ref,
    lead_ref, ar_ref, ac_ref, w_ref, u_ref, g_ref, *, scale, quarters,
):
    r = at_ref[0]
    c = at_ref[1]
    even = at_ref[2] == 0
    grid, tokens, _ = cols_ref.shape
    part = tokens // quarters
    block = grid * part

    def eye(n):
        i = lax.broadcasted_iota(jnp.int32, (n, n), 0)
        j = lax.broadcasted_iota(jnp.int32, (n, n), 1)
        return i == j

    for q in range(quarters):
        for h in range(2):
            x = h * quarters + q
            mine = mine_ref[x, :block, :]
            other = other_ref[x, :block, :]
            lead_ref[q * block : (q + 1) * block, h * BS : (h + 1) * BS] = jnp.where(even, mine, other)
            lead_ref[q * block : (q + 1) * block, NB + h * BS : NB + (h + 1) * BS] = jnp.where(even, other, mine)
    for t in range(grid):
        for q in range(quarters):
            to = slice(q * block + t * part, q * block + (t + 1) * part)
            ac_ref[to, :] = cols_ref[t, q * part : (q + 1) * part, :]
            for h in range(2):
                at = block + h * tokens + q * part
                mine = mine_ref[t // 2, at : at + part, :]
                other = other_ref[t // 2, at : at + part, :]
                same = even if t % 2 == 0 else jnp.logical_not(even)
                ar_ref[to, h * BS : (h + 1) * BS] = jnp.where(same, mine, other)

    lead = lead_ref[...]
    w_ref[:, :LEAD] = tdot(lead, lead) * scale + jnp.where(eye(LEAD), dlead_ref[...], 0.0)
    w_ref[:, LEAD : LEAD + NB] = tdot(lead, ar_ref[...]) * scale
    w_ref[:, LEAD + NB :] = tdot(lead, ac_ref[...]) * scale

    steps = LEAD // BS

    def step(b, carry):
        for k in range(steps):
            @pl.when(b == k)
            def _():
                g_ref[:, :BS] = w_ref[k * BS : (k + 1) * BS, k * BS : (k + 1) * BS]
        g_ref[:, BS:] = jnp.where(eye(BS), 1.0, 0.0).astype(jnp.float32)
        factor_block(g_ref)
        for k in range(steps):
            @pl.when(b == k)
            def _():
                here = slice(k * BS, (k + 1) * BS)
                after = (k + 1) * BS
                u = jnp.dot(
                    g_ref[:, BS:], w_ref[here, after:], precision=HIGHEST, preferred_element_type=jnp.float32
                )
                u_ref[here, here] = g_ref[:, :BS]
                u_ref[here, after:] = u
                if after < LEAD:
                    w_ref[after:LEAD, after:] -= tdot(u[:, : LEAD - after], u, HIGHEST)
        return carry

    lax.fori_loop(0, steps, step, 0)

    i = lax.broadcasted_iota(jnp.int32, (NB, NB), 0)
    j = lax.broadcasted_iota(jnp.int32, (NB, NB), 1)

    @pl.when((c >= PANELS) & (r >= PANELS))
    def _():
        own = tdot(ar_ref[...], ac_ref[...]) * scale
        own = own + jnp.where((i == j) & (r == c), down_ref[...], 0.0)
        o_ref[...] = own - tdot(u_ref[:, LEAD : LEAD + NB], u_ref[:, LEAD + NB :], HIGHEST)

    @pl.when((r < PANELS) & (c > r))
    def _():
        o_ref[...] = jnp.zeros((NB, NB), jnp.float32)

    for p in range(PANELS):
        here = slice(p * NB, (p + 1) * NB)

        @pl.when((c == p) & (r == p))
        def _():
            o_ref[:BS, :BS] = u_ref[p * NB : p * NB + BS, p * NB : p * NB + BS].T
            o_ref[:BS, BS:] = jnp.zeros((BS, BS), jnp.float32)
            o_ref[BS:, :BS] = u_ref[p * NB : p * NB + BS, p * NB + BS : (p + 1) * NB].T
            o_ref[BS:, BS:] = u_ref[p * NB + BS : (p + 1) * NB, p * NB + BS : (p + 1) * NB].T
            o_ref[...] = jnp.where(i >= j, o_ref[...], 0.0)

        @pl.when((c == p) & (r > p))
        def _():
            o_ref[...] = u_ref[here, LEAD : LEAD + NB].T


def local_part(at, mine, other, cols, dlead, down, scale, quarters):
    vmem = pl.BlockSpec(memory_space=pltpu.VMEM)
    total = cols.shape[0] * cols.shape[1]
    return pl.pallas_call(
        functools.partial(local_kernel, scale=scale, quarters=quarters),
        out_shape=jax.ShapeDtypeStruct((NB, NB), jnp.float32),
        in_specs=[pl.BlockSpec(memory_space=pltpu.SMEM)] + [vmem] * 5,
        out_specs=vmem,
        scratch_shapes=[
            pltpu.VMEM((total, LEAD), jnp.bfloat16),
            pltpu.VMEM((total, NB), jnp.bfloat16),
            pltpu.VMEM((total, NB), jnp.bfloat16),
            pltpu.VMEM((LEAD, LEAD + 2 * NB), jnp.float32),
            pltpu.VMEM((LEAD, LEAD + 2 * NB), jnp.float32),
            pltpu.VMEM((BS, 2 * BS), jnp.float32),
        ],
        compiler_params=pltpu.CompilerParams(vmem_limit_bytes=24 * 2**20),
    )(at, mine, other, cols, dlead, down)


def to_all(shard, axis, copies, groups=None):
    shards = jnp.broadcast_to(shard, (copies, *shard.shape))
    return lax.all_to_all(shards, axis, 0, 0, axis_index_groups=groups, tiled=True)


def on_device(activations, damping):
    tokens, width = activations.shape
    grid = lax.axis_size("row")
    cores = 2
    chips = lax.axis_size("col") // cores
    halves = width // BS
    quarters = chips // halves
    part = tokens // quarters
    row_dev = lax.axis_index("row")
    col_dev = lax.axis_index("col")
    core = col_dev % cores
    same_core = [[x * cores + k for x in range(chips)] for k in range(cores)]
    transpose = [(r * grid + c, c * grid + r) for r in range(grid) for c in range(grid)]

    def by_half(x):
        return x.reshape(tokens, halves, BS).transpose(1, 0, 2)

    turned = lax.ppermute(activations, ("row", "col"), transpose)
    lead_piece = lax.all_to_all(
        by_half(activations).reshape(chips, part, BS), "col", 0, 0, axis_index_groups=same_core, tiled=True
    )[0]

    d0 = lax.reduce_precision(damping, 8, 7)
    d1 = lax.reduce_precision(damping - d0, 8, 7)
    d2 = damping - d0 - d1
    damp_rows = jnp.stack([d0, d1, d2, jnp.zeros_like(d2)]).astype(jnp.bfloat16).reshape(4 * halves, BS)
    pieces = to_all(jnp.concatenate([lead_piece, damp_rows]), "row", grid)
    damp = pieces[:PANELS, part:].reshape(PANELS, 4, width).astype(jnp.float32)
    damp = ((damp[:, 2] + damp[:, 1]) + damp[:, 0]).reshape(1, PANELS * width)

    own, pieces = lax.optimization_barrier((activations, pieces))
    sent = jnp.concatenate([pieces[:, :part].reshape(grid * part, BS), by_half(turned).reshape(halves * tokens, BS)])
    mine = to_all(sent, "col", chips, same_core)
    cols = lax.all_gather(own, "row")
    other = lax.ppermute(mine, "col", [(c, c ^ 1) for c in range(chips * cores)])
    at = jnp.stack([row_dev, col_dev, core]).astype(jnp.int32)
    return local_part(
        at, mine, other, cols, damp, damping.reshape(1, width), 1.0 / (tokens * grid), quarters
    )


def solution(mesh):
    in_specs = (P(("groups", "row"), "col"), P(("groups", "row")))
    out_specs = P(("groups", "row"), "col")
    return jax.shard_map(
        on_device, mesh=mesh, in_specs=in_specs, out_specs=out_specs, check_vma=False
    )
```

```python
import functools

import jax
import jax.numpy as jnp
from jax import lax
from jax.experimental import pallas as pl
from jax.experimental.pallas import tpu as pltpu
from jax.sharding import PartitionSpec as P


NB = 256
PANELS = 2
LEAD = NB * PANELS
BS = 128
SUB = 8

HIGHEST = lax.Precision.HIGHEST


def tdot(a, b, precision=None):
    return lax.dot_general(
        a, b, (((0,), (0,)), ((), ())), precision=precision, preferred_element_type=jnp.float32
    )


def both(x):
    return jnp.concatenate([x, x], 1)


def lanes(g, at):
    return [jnp.broadcast_to(g[:, at + j : at + j + 1], (SUB, BS)) for j in range(SUB)]


def sublane(x, m):
    return jnp.broadcast_to(x[m : m + 1, :], (SUB, x.shape[1]))


def factor_block(g_ref):
    sub = lax.broadcasted_iota(jnp.int32, (SUB, BS), 0)
    sub2 = lax.broadcasted_iota(jnp.int32, (SUB, 2 * BS), 0)
    strips = BS // SUB
    half = strips // 2
    for k in range(strips):
        at = SUB * k
        end = (k // half + 1) * half
        if k % half == 0:
            if k > 0:
                g_ref[at:, :] -= tdot(g_ref[:at, at:BS], g_ref[:at, :], HIGHEST)
            rows = g_ref[at : at + SUB, :]
            cols = lanes(rows, at)
        ahead = k + 1 < end
        if ahead:
            next_rows = g_ref[at + SUB : at + 2 * SUB, :]
            low = lanes(next_rows, at)
            next_cols = lanes(next_rows, at + SUB)
        out = rows
        for j in range(SUB):
            d = sublane(cols[j], j)
            rc = 1.0 / d
            rs = lax.rsqrt(d)
            t = {m: sublane(cols[j], m) * rc for m in range(j + 1, SUB)}
            if ahead:
                for n in range(SUB):
                    next_cols[n] = next_cols[n] - low[j] * (sublane(low[j], n) * rc)
                for m in range(j + 1, SUB):
                    low[m] = low[m] - low[j] * t[m]
            for m in range(j + 1, SUB):
                cols[m] = jnp.where(sub == j, t[m], cols[m] - cols[j] * t[m])
            row = sublane(rows, j)
            out = jnp.where(sub2 == j, row * both(rs), out)
            w = row * both(rc)
            rows = jnp.where(sub2 == j, w, rows - both(cols[j]) * w)
            if ahead:
                next_rows = next_rows - both(low[j]) * w
        g_ref[at : at + SUB, :] = out
        if k + 2 < end:
            solved = [sublane(rows, j) for j in range(SUB)]
            for i in range(k + 2, end):
                acc = g_ref[i * SUB : (i + 1) * SUB, :]
                for a, y in zip(lanes(acc, at), solved, strict=True):
                    acc = acc - both(a) * y
                g_ref[i * SUB : (i + 1) * SUB, :] = acc
        if ahead:
            rows, cols = next_rows, next_cols


def local_kernel(
    at_ref, mine_ref, other_ref, cols_ref, dlead_ref, down_ref, o_ref,
    lead_ref, ar_ref, ac_ref, w_ref, u_ref, g_ref, own_ref, *, scale, quarters,
):
    r = at_ref[0]
    c = at_ref[1]
    even = at_ref[2] == 0
    grid, tokens, _ = cols_ref.shape
    part = tokens // quarters
    block = grid * part

    def eye(n):
        i = lax.broadcasted_iota(jnp.int32, (n, n), 0)
        j = lax.broadcasted_iota(jnp.int32, (n, n), 1)
        return i == j

    for q in range(quarters):
        for h in range(2):
            x = h * quarters + q
            mine = mine_ref[x, :block, :]
            other = other_ref[x, :block, :]
            lead_ref[q * block : (q + 1) * block, h * BS : (h + 1) * BS] = jnp.where(even, mine, other)
            lead_ref[q * block : (q + 1) * block, NB + h * BS : NB + (h + 1) * BS] = jnp.where(even, other, mine)
    for t in range(grid):
        for q in range(quarters):
            to = slice(q * block + t * part, q * block + (t + 1) * part)
            ac_ref[to, :] = cols_ref[t, q * part : (q + 1) * part, :]
            for h in range(2):
                at = block + h * tokens + q * part
                mine = mine_ref[t // 2, at : at + part, :]
                other = other_ref[t // 2, at : at + part, :]
                same = even if t % 2 == 0 else jnp.logical_not(even)
                ar_ref[to, h * BS : (h + 1) * BS] = jnp.where(same, mine, other)

    lead = lead_ref[...]
    w_ref[:, :LEAD] = tdot(lead, lead) * scale + jnp.where(eye(LEAD), dlead_ref[...], 0.0)
    w_ref[:, LEAD : LEAD + NB] = tdot(lead, ar_ref[...]) * scale
    w_ref[:, LEAD + NB :] = tdot(lead, ac_ref[...]) * scale
    own_ref[...] = tdot(ar_ref[...], ac_ref[...]) * scale

    steps = LEAD // BS
    for k in range(steps):
        g = g_ref.at[k]
        here = slice(k * BS, (k + 1) * BS)
        after = (k + 1) * BS
        g[:, :BS] = w_ref[here, here]
        g[:, BS:] = jnp.where(eye(BS), 1.0, 0.0).astype(jnp.float32)
        factor_block(g)
        u_ref[here, here] = g[:, :BS]
        inverse = g[:, BS:]
        if after < LEAD:
            near = slice(after, after + BS)
            u = jnp.dot(inverse, w_ref[here, near], precision=HIGHEST, preferred_element_type=jnp.float32)
            u_ref[here, near] = u
            w_ref[near, near] -= tdot(u, u, HIGHEST)
        far = min(after + BS, LEAD)
        v = jnp.dot(inverse, w_ref[here, far:], precision=HIGHEST, preferred_element_type=jnp.float32)
        u_ref[here, far:] = v
        if after < LEAD:
            w_ref[near, far:] -= tdot(u, v, HIGHEST)
            if far < LEAD:
                w_ref[far:LEAD, far:] -= tdot(v[:, : LEAD - far], v, HIGHEST)
        own_ref[...] -= tdot(v[:, LEAD - far : LEAD - far + NB], v[:, LEAD - far + NB :], HIGHEST)

    i = lax.broadcasted_iota(jnp.int32, (NB, NB), 0)
    j = lax.broadcasted_iota(jnp.int32, (NB, NB), 1)

    @pl.when((c >= PANELS) & (r >= PANELS))
    def _():
        o_ref[...] = own_ref[...] + jnp.where((i == j) & (r == c), down_ref[...], 0.0)

    @pl.when((r < PANELS) & (c > r))
    def _():
        o_ref[...] = jnp.zeros((NB, NB), jnp.float32)

    for p in range(PANELS):
        here = slice(p * NB, (p + 1) * NB)

        @pl.when((c == p) & (r == p))
        def _():
            o_ref[:BS, :BS] = u_ref[p * NB : p * NB + BS, p * NB : p * NB + BS].T
            o_ref[:BS, BS:] = jnp.zeros((BS, BS), jnp.float32)
            o_ref[BS:, :BS] = u_ref[p * NB : p * NB + BS, p * NB + BS : (p + 1) * NB].T
            o_ref[BS:, BS:] = u_ref[p * NB + BS : (p + 1) * NB, p * NB + BS : (p + 1) * NB].T
            o_ref[...] = jnp.where(i >= j, o_ref[...], 0.0)

        @pl.when((c == p) & (r > p))
        def _():
            o_ref[...] = u_ref[here, LEAD : LEAD + NB].T


def local_part(at, mine, other, cols, dlead, down, scale, quarters):
    vmem = pl.BlockSpec(memory_space=pltpu.VMEM)
    total = cols.shape[0] * cols.shape[1]
    return pl.pallas_call(
        functools.partial(local_kernel, scale=scale, quarters=quarters),
        out_shape=jax.ShapeDtypeStruct((NB, NB), jnp.float32),
        in_specs=[pl.BlockSpec(memory_space=pltpu.SMEM)] + [vmem] * 5,
        out_specs=vmem,
        scratch_shapes=[
            pltpu.VMEM((total, LEAD), jnp.bfloat16),
            pltpu.VMEM((total, NB), jnp.bfloat16),
            pltpu.VMEM((total, NB), jnp.bfloat16),
            pltpu.VMEM((LEAD, LEAD + 2 * NB), jnp.float32),
            pltpu.VMEM((LEAD, LEAD + 2 * NB), jnp.float32),
            pltpu.VMEM((LEAD // BS, BS, 2 * BS), jnp.float32),
            pltpu.VMEM((NB, NB), jnp.float32),
        ],
        compiler_params=pltpu.CompilerParams(vmem_limit_bytes=14 * 2**20),
    )(at, mine, other, cols, dlead, down)


def to_all(shard, axis, copies, groups=None):
    shards = jnp.broadcast_to(shard, (copies, *shard.shape))
    return lax.all_to_all(shards, axis, 0, 0, axis_index_groups=groups, tiled=True)


def on_device(activations, damping):
    tokens, width = activations.shape
    grid = lax.axis_size("row")
    cores = 2
    chips = lax.axis_size("col") // cores
    halves = width // BS
    quarters = chips // halves
    part = tokens // quarters
    row_dev = lax.axis_index("row")
    col_dev = lax.axis_index("col")
    core = col_dev % cores
    same_core = [[x * cores + k for x in range(chips)] for k in range(cores)]
    transpose = [(r * grid + c, c * grid + r) for r in range(grid) for c in range(grid)]

    def by_half(x):
        return jnp.concatenate([x[:, h * BS : (h + 1) * BS] for h in range(halves)])

    turned = lax.ppermute(activations, ("row", "col"), transpose)
    lead_piece = lax.all_to_all(
        by_half(activations).reshape(chips, part, BS), "col", 0, 0, axis_index_groups=same_core, tiled=True
    )[0]

    d0 = lax.reduce_precision(damping, 8, 7)
    d1 = lax.reduce_precision(damping - d0, 8, 7)
    d2 = damping - d0 - d1
    damp_rows = jnp.stack([d0, d1, d2, jnp.zeros_like(d2)]).astype(jnp.bfloat16).reshape(4 * halves, BS)
    pieces = to_all(jnp.concatenate([lead_piece, damp_rows]), "row", grid)
    damp = pieces[:PANELS, part:].reshape(PANELS, 4, width).astype(jnp.float32)
    damp = ((damp[:, 2] + damp[:, 1]) + damp[:, 0]).reshape(1, PANELS * width)

    own, pieces = lax.optimization_barrier((activations, pieces))
    sent = jnp.concatenate([pieces[:, :part].reshape(grid * part, BS), by_half(turned).reshape(halves * tokens, BS)])
    mine = to_all(sent, "col", chips, same_core)
    cols = lax.all_gather(own, "row")
    other = lax.ppermute(mine, "col", [(c, c ^ 1) for c in range(chips * cores)])
    at = jnp.stack([row_dev, col_dev, core]).astype(jnp.int32)
    return local_part(
        at, mine, other, cols, damp, damping.reshape(1, width), 1.0 / (tokens * grid), quarters
    )


def solution(mesh):
    in_specs = (P(("groups", "row"), "col"), P(("groups", "row")))
    out_specs = P(("groups", "row"), "col")
    return jax.shard_map(
        on_device, mesh=mesh, in_specs=in_specs, out_specs=out_specs, check_vma=False
    )
```
